32 devices in a mesh: groups: 2 (over y), ep: 4 (over x, core), tp: 4 (over z).
Axes of the slice: x: 2, y: 2, z: 4, core: 2. Of those that a mesh axis runs over, the one named last changes fastest.
Arguments:
- hidden_states: bfloat16 [256, 7168], P(('groups', 'ep', 'tp')), parts along dimension 0, may hold values from -6 to 6
- norm_gain: float32 [7168], replicated, may hold values from 0.1 to 1.9
- expert_ids: int32 [256, 8], P(('groups', 'ep', 'tp')), parts along dimension 0, may hold values from 0 to 15, all different within a row; in each aligned block of 8 rows (0 to 7, 8 to 15, ...) at most 5 rows name the same one
- gate_weights: float32 [256, 8], P(('groups', 'ep', 'tp')), parts along dimension 0, may hold values from 0.1 to 1
- capacity: int32 [16], replicated, may hold values from 3 to 5
- expert_in: bfloat16 [16, 2048, 2, 7168], P('ep', 'tp'), may hold values from -0.0625 to 0.0625
- expert_out: bfloat16 [16, 2048, 7168], P('ep', 'tp'), may hold values from -0.125 to 0.125
Outputs:
- mixed_out: bfloat16 [256, 7168], P(('groups', 'ep', 'tp')), parts along dimension 0
The draws below stay inside these ranges and needn't reach their ends.
There are 2 independent parts, one for each index of `groups`. The reference program is written for one: setup_inputs(seed, part) draws one part's arguments, and reference() takes and returns one part's arrays. A program takes and returns all parts, laid end to end along the dimension named above; an argument that names none is the same for every part. Nothing has to cross between parts.
Inputs may be any that keep to these rules, and one draw needn't show every extreme that they name: `expert_ids`: each row names 8 different experts; within the rows of one device no expert is named more than 5 times.
All inputs are finite; a program needn't handle non-finite values.
Results may differ from the reference program's by a relative error of at most 0.006.
Values may be sent and summed in bfloat16 or wider, within the bound.
A program may use at most 320 MiB of HBM per device.

```python
import math
import jax
import jax.numpy as jnp
import numpy as np
from jax import lax

D = 7168
F = 2048
TOPK = 8
EXPERTS = 16
TOK_DEV = 8
CAP = 5
TOKENS = 128
N_EP = 4
N_TP = 4


def touch_ends(result, rng, least, top_value):
    dims = result.shape
    index_at = [jax.random.randint(jax.random.fold_in(rng, axis), (), 0, dims[axis]) for axis in range(len(dims))]
    result = result.at[tuple(index_at)].set(least)
    longest = dims.index(max(dims))
    index_at[longest] = (index_at[longest] + 1) % dims[longest]
    return result.at[tuple(index_at)].set(top_value)


def steps_of(rng, extent, split, least, largest):
    factor_of, own = 1.0, jax.random.fold_in(rng, 6)
    for axis_at, blocks in split:
        draws = jnp.exp(jax.random.uniform(jax.random.fold_in(own, axis_at), (blocks,), jnp.float32, least / len(split), largest / len(split)))
        factor_of = factor_of * jnp.repeat(draws, extent[axis_at] // blocks).reshape([-1 if axis == axis_at else 1 for axis in range(len(extent))])
    return factor_of


def assign_block(stream_key, own, number, rows, number_of, top, reach, slope):
    order = jax.random.permutation(stream_key, number_of)
    packed, ordinary = shares(number_of, rows * top, reach, slope, True), shares(number_of, rows * top, reach, slope, False)
    places = jnp.arange(number_of)

    def named(lengths, offset_by):
        used = int((lengths > 0).sum())
        fixed = max(1, used // 4)
        passed = fixed + (places - fixed + offset_by * (used - fixed)) % max(1, number_of - fixed)
        return jnp.zeros((number_of,), jnp.int32).at[order[jnp.where(places < fixed, places, passed)]].set(jnp.asarray(lengths, jnp.int32))

    lengths = jnp.where(number % 4 == 0, named(packed, number // 4), named(ordinary, number - number // 4 - 1))
    mixed = jax.random.permutation(jax.random.fold_in(own, 3), number_of)
    giver, taker = mixed[0:number_of // 2 * 2:2], mixed[1:number_of // 2 * 2:2]
    margin = jnp.minimum(lengths[giver] - 1, reach - lengths[taker]) // 2
    margin = jnp.where((giver == order[0]) | (taker == order[0]) | (lengths[taker] == 0), 0, jnp.maximum(margin, 0))
    passed = jax.random.randint(jax.random.fold_in(own, 4), (number_of // 2,), 0, 1 << 20) % (margin + 1)
    lengths = lengths.at[giver].add(-passed).at[taker].add(passed)
    members = jnp.searchsorted(jnp.cumsum(lengths), jnp.arange(rows * top), side="right").astype(jnp.int32)
    table = members.reshape(top, rows).T
    table = table[jax.random.permutation(jax.random.fold_in(own, 1), rows)]
    offset_by = jax.random.randint(jax.random.fold_in(own, 2), (rows, 1), 0, top)
    return jnp.take_along_axis(table, (jnp.arange(top)[None, :] + offset_by) % top, axis=1)


def shares(number_of, total, reach, slope, full):
    portions = [(1 << 20) // math.isqrt(rank ** slope) + 1 for rank in range(1, number_of + 1)]
    largest = reach if full else min(reach, max(-(-total // number_of), total * portions[0] // sum(portions)))
    least = 1 if total - largest >= number_of - 1 else 0
    given, surplus = [largest] + [least] * (number_of - 1), total - largest - least * (number_of - 1)
    while surplus > 0:
        candidates = [i for i in range(1, number_of) if given[i] < largest] or [i for i in range(1, number_of) if given[i] < reach]
        pool, budget = sum([portions[i] for i in candidates]), surplus
        for i in candidates:
            extra = min(reach - given[i], max(1, budget * portions[i] // pool), surplus)
            given[i] = given[i] + extra
            surplus = surplus - extra
    return np.array(given)


def scatter_about(key, shape, width, limit, split=(), held_as=jnp.bfloat16):
    loudness = steps_of(key, shape, split, -0.22, 0.18) if split else 1.0
    array = jax.random.normal(key, shape, jnp.float32) * width * loudness
    return jnp.minimum(jnp.maximum(array, -limit), limit).astype(held_as)


def setup_inputs(seed: int = 0, part: int = 0) -> dict:
    arg_keys = jax.random.split(jax.random.key(seed), 8)
    own_keys = jax.random.split(jax.random.fold_in(arg_keys[7], part), 8)
    hidden_states = scatter_about(own_keys[0], (TOKENS, D), 1.0, 6.0, ((0, 16),))
    norm_gain = jnp.clip(1.0 + 0.18 * jax.random.normal(arg_keys[1], (D,), jnp.float32), 0.1, 1.9)
    expert_ids_keys = jax.random.split(jax.random.fold_in(own_keys[2], 1), TOKENS // TOK_DEV)
    expert_ids_turns = jax.random.permutation(jax.random.fold_in(own_keys[2], 3), TOKENS // TOK_DEV)
    expert_ids = jax.vmap(lambda own, number: assign_block(jax.random.fold_in(own_keys[2], 2), own, number, TOK_DEV, EXPERTS, TOPK, CAP, 1))(expert_ids_keys, expert_ids_turns).reshape((TOKENS, TOPK))
    gate_weights = jnp.clip(jnp.exp(math.log(1.0) - 2.3025851 * jax.random.uniform(own_keys[3], (TOKENS, TOPK), jnp.float32) ** steps_of(own_keys[3], (TOKENS, TOPK), ((0, 16),), -0.2, 0.2)), 0.1, 1.0)
    capacity = touch_ends(jax.random.randint(arg_keys[4], (EXPERTS,), max(1, CAP - 2), CAP + 1), jax.random.fold_in(arg_keys[4], 1), max(1, CAP - 2), CAP).astype(jnp.int32)
    expert_in = scatter_about(arg_keys[5], (EXPERTS, F, 2, D), D ** -0.5, 0.0625, ((0, 4), (1, 4)))
    expert_out = scatter_about(arg_keys[6], (EXPERTS, F, D), F ** -0.5, 0.125, ((0, 4), (1, 4)))
    return {"hidden_states": hidden_states, "norm_gain": norm_gain, "expert_ids": expert_ids, "gate_weights": gate_weights, "capacity": capacity, "expert_in": expert_in, "expert_out": expert_out}


EPSILON = 1e-06

def reference(hidden_states, norm_gain, expert_ids, gate_weights, capacity, expert_in, expert_out):
    device_count = N_EP * N_TP
    route_count = TOK_DEV * TOPK
    values = hidden_states.astype(jnp.float32)
    inverse = lax.rsqrt(lax.optimization_barrier(jnp.mean(values * values, axis=1, keepdims=True)) + EPSILON)
    normed = (values * inverse * norm_gain).astype(jnp.bfloat16)
    route_ids = expert_ids.reshape(device_count, route_count)
    onehot = (route_ids[:, :, None] == jnp.arange(EXPERTS, dtype=jnp.int32)[None, None, :]).astype(jnp.int32)
    before = lax.optimization_barrier(jnp.sum((jnp.cumsum(onehot, axis=1) - onehot) * onehot, axis=2))
    keeping = before < capacity[route_ids]
    device_index = jnp.arange(device_count, dtype=jnp.int32)[:, None]
    token_index = device_index * TOK_DEV + jnp.arange(route_count, dtype=jnp.int32)[None, :] // TOPK
    dump_slot = device_count * CAP
    position = jnp.where(keeping, device_index * CAP + before, dump_slot).astype(jnp.int32)
    table = jnp.full((EXPERTS, dump_slot + 1), TOKENS, jnp.int32)
    table = table.at[route_ids, position].set(jnp.where(keeping, token_index, TOKENS).astype(jnp.int32))
    padded = jnp.concatenate([normed, jnp.zeros((1, D), normed.dtype)], axis=0)

    def one_expert(operands):
        weight_in, weight_out, index = operands
        row_block = padded[index]
        gate_part = jnp.dot(row_block, weight_in[:, 0, :].T, preferred_element_type=jnp.float32)
        up_part = jnp.dot(row_block, weight_in[:, 1, :].T, preferred_element_type=jnp.float32)
        hidden = (jax.nn.silu(gate_part) * up_part).astype(jnp.bfloat16)
        return jnp.dot(hidden, weight_out, preferred_element_type=jnp.float32).astype(jnp.bfloat16)
    answers = lax.map(one_expert, (expert_in, expert_out, table))
    picked = answers[route_ids, position].astype(jnp.float32)
    weighting = jnp.where(keeping, gate_weights.reshape(device_count, route_count), 0.0).astype(jnp.float32)
    terms = (picked * weighting[:, :, None]).reshape(device_count, TOK_DEV, TOPK, D)
    branch_sum = lax.optimization_barrier(jnp.sum(terms, axis=2)).reshape(TOKENS, D)
    return (values + branch_sum).astype(jnp.bfloat16)
```

```python
import functools
import jax
import jax.numpy as jnp
from jax import lax
from jax.experimental import pallas as pl
from jax.experimental.pallas import tpu as pltpu
from jax.sharding import PartitionSpec as P

EPSILON = 1e-06
ROWS = 128


def experts_kernel(x_ref, w_ref, in_hbm, out_w_ref, o_ref, stage, pair, total, sems):
    e, f = pl.program_id(1), pl.program_id(2)
    n_e, n_f = pl.num_programs(1), pl.num_programs(2)
    step = e * n_f + f
    last = n_e * n_f
    block = stage.shape[1]
    flat = in_hbm.reshape(in_hbm.shape[0] * in_hbm.shape[1] * 2, in_hbm.shape[3])

    def fetch(at):
        return pltpu.make_async_copy(
            flat.at[pl.ds(pl.multiple_of(at * block, block), block)], stage.at[at % 2], sems.at[at % 2]
        )

    @pl.when(step == 0)
    def _():
        fetch(step).start()

    @pl.when(step + 1 < last)
    def _():
        fetch(step + 1).start()

    fetch(step).wait()
    pair[...] = lax.dot_general(
        stage[step % 2], x_ref[...], (((1,), (1,)), ((), ())), preferred_element_type=jnp.float32
    )
    half = block // 2
    gate = pair[pl.ds(0, half, stride=2), :]
    up = pair[pl.ds(1, half, stride=2), :]
    scale = w_ref[pl.ds(e, 1), :]
    hidden = gate / (1.0 + jnp.exp(-gate)) * up * scale
    hidden = hidden.T.astype(jnp.bfloat16)
    part = jnp.dot(hidden, out_w_ref[0], preferred_element_type=jnp.float32)

    @pl.when(step == 0)
    def _():
        total[...] = part

    @pl.when(step > 0)
    def _():
        total[...] += part

    @pl.when(step == last - 1)
    def _():
        o_ref[...] = total[...].astype(o_ref.dtype)


def experts(x, weights, expert_in, expert_out):
    count, width = x.shape
    n_e, n_f = expert_in.shape[:2]
    block = min(256, n_f)
    return pl.pallas_call(
        experts_kernel,
        grid=(count // ROWS, n_e, n_f // block),
        out_shape=jax.ShapeDtypeStruct((count, width), jnp.bfloat16),
        in_specs=[
            pl.BlockSpec((ROWS, width), lambda t, e, f: (t, 0)),
            pl.BlockSpec((weights.shape[0], ROWS), lambda t, e, f: (0, t)),
            pl.BlockSpec(memory_space=pl.ANY),
            pl.BlockSpec((1, block, width), lambda t, e, f: (e, f, 0)),
        ],
        out_specs=pl.BlockSpec((ROWS, width), lambda t, e, f: (t, 0)),
        scratch_shapes=[
            pltpu.VMEM((2, 2 * block, width), jnp.bfloat16),
            pltpu.VMEM((2 * block, ROWS), jnp.float32),
            pltpu.VMEM((ROWS, width), jnp.float32),
            pltpu.SemaphoreType.DMA((2,)),
        ],
        compiler_params=pltpu.CompilerParams(vmem_limit_bytes=60 * 2**20),
    )(x, weights, expert_in, expert_out)


def shards(hidden_states, norm_gain, expert_ids, gate_weights, capacity, expert_in, expert_out):
    token_count, width = hidden_states.shape
    expert_count = capacity.shape[0]
    local_count = expert_in.shape[0]
    values = hidden_states.astype(jnp.float32)
    inverse = lax.rsqrt(jnp.mean(values * values, axis=1, keepdims=True) + EPSILON)
    normed = (values * inverse * norm_gain).astype(jnp.bfloat16)
    lanes = jnp.arange(expert_count, dtype=jnp.int32)
    chosen = (expert_ids[:, :, None] == lanes).astype(jnp.float32)
    named = jnp.sum(chosen, axis=1)
    lower = jnp.tril(jnp.ones((token_count, token_count), jnp.float32), -1)
    before = jnp.dot(lower, named, precision=lax.Precision.HIGHEST)
    kept = before < capacity[None, :].astype(jnp.float32)
    gates = jnp.where(kept, jnp.sum(chosen * gate_weights[:, :, None], axis=1), 0.0)
    high = gates.astype(jnp.bfloat16)
    low = (gates - high.astype(jnp.float32)).astype(jnp.bfloat16)
    pad = jnp.zeros((token_count, 128 - 2 * expert_count), jnp.bfloat16)
    sent = jnp.concatenate([normed, high, low, pad], axis=1)
    gathered = lax.all_gather(sent, ("ep", "tp"), axis=0, tiled=True)
    x = gathered[:, :width]
    high = gathered[:, width : width + expert_count].astype(jnp.float32)
    low = gathered[:, width + expert_count : width + 2 * expert_count].astype(jnp.float32)
    mine = lax.dynamic_slice_in_dim(high + low, lax.axis_index("ep") * local_count, local_count, 1)
    part = experts(x, mine.T, expert_in, expert_out)
    summed = lax.psum_scatter(part, ("ep", "tp"), scatter_dimension=0, tiled=True)
    return (values + summed.astype(jnp.float32)).astype(jnp.bfloat16)


def solution(mesh):
    in_specs = (
        P(("groups", "ep", "tp"), None),
        P(),
        P(("groups", "ep", "tp"), None),
        P(("groups", "ep", "tp"), None),
        P(),
        P("ep", "tp", None, None),
        P("ep", "tp", None),
    )
    out_specs = P(("groups", "ep", "tp"), None)
    return jax.shard_map(shards, mesh=mesh, in_specs=in_specs, out_specs=out_specs, check_vma=False)
```

```python
import jax
import jax.numpy as jnp
from jax import lax
from jax.experimental import pallas as pl
from jax.experimental.pallas import tpu as pltpu
from jax.sharding import PartitionSpec as P

EPSILON = 1e-06
ROWS = 128


def experts_kernel(x_ref, w_ref, in_hbm, out_w_ref, o_ref, stage, pair, total, sems):
    e, f = pl.program_id(1), pl.program_id(2)
    n_e, n_f = pl.num_programs(1), pl.num_programs(2)
    step = e * n_f + f
    last = n_e * n_f
    block = stage.shape[1]
    flat = in_hbm.reshape(in_hbm.shape[0] * in_hbm.shape[1] * 2, in_hbm.shape[3])

    def fetch(at):
        return pltpu.make_async_copy(
            flat.at[pl.ds(pl.multiple_of(at * block, block), block)], stage.at[at % 2], sems.at[at % 2]
        )

    @pl.when(step == 0)
    def _():
        fetch(step).start()

    @pl.when(step + 1 < last)
    def _():
        fetch(step + 1).start()

    fetch(step).wait()
    pair[...] = lax.dot_general(
        stage[step % 2], x_ref[...], (((1,), (1,)), ((), ())), preferred_element_type=jnp.float32
    )
    half = block // 2
    gate = pair[pl.ds(0, half, stride=2), :]
    up = pair[pl.ds(1, half, stride=2), :]
    scale = w_ref[pl.ds(e, 1), :]
    hidden = gate / (1.0 + jnp.exp(-gate)) * up * scale
    hidden = hidden.T.astype(jnp.bfloat16)
    part = jnp.dot(hidden, out_w_ref[0], preferred_element_type=jnp.float32)

    @pl.when(step == 0)
    def _():
        total[...] = part

    @pl.when(step > 0)
    def _():
        total[...] += part

    @pl.when(step == last - 1)
    def _():
        o_ref[...] = total[...].astype(o_ref.dtype)


def experts(x, width, weights, expert_in, expert_out):
    count = x.shape[0]
    n_e, n_f = expert_in.shape[:2]
    block = min(256, n_f)
    return pl.pallas_call(
        experts_kernel,
        grid=(count // ROWS, n_e, n_f // block),
        out_shape=jax.ShapeDtypeStruct((count, width), jnp.bfloat16),
        in_specs=[
            pl.BlockSpec((ROWS, width), lambda t, e, f: (t, 0)),
            pl.BlockSpec((weights.shape[0], ROWS), lambda t, e, f: (0, t)),
            pl.BlockSpec(memory_space=pl.ANY),
            pl.BlockSpec((1, block, width), lambda t, e, f: (e, f, 0)),
        ],
        out_specs=pl.BlockSpec((ROWS, width), lambda t, e, f: (t, 0)),
        scratch_shapes=[
            pltpu.VMEM((2, 2 * block, width), jnp.bfloat16),
            pltpu.VMEM((2 * block, ROWS), jnp.float32),
            pltpu.VMEM((ROWS, width), jnp.float32),
            pltpu.SemaphoreType.DMA((2,)),
        ],
        compiler_params=pltpu.CompilerParams(vmem_limit_bytes=60 * 2**20),
    )(x, weights, expert_in, expert_out)


MESH = pl.DeviceIdType.MESH


def places():
    n_x, n_z = lax.axis_size("ep") // 2, lax.axis_size("tp")
    ep, z = lax.axis_index("ep"), lax.axis_index("tp")
    return n_x, n_z, ep // 2, ep % 2, z


def greet(n_x, n_z, x, c, z):
    barrier = pltpu.get_barrier_semaphore()
    peers = [(x, 1 - c, z)]
    peers += [((x + d) % n_x, c, z) for d in range(1, n_x)]
    peers += [(x, c, (z + k) % n_z) for k in range(1, n_z)]
    for px, pc, pz in peers:
        pl.semaphore_signal(barrier, inc=1, device_id={"ep": px * 2 + pc, "tp": pz}, device_id_type=MESH)
    pl.semaphore_wait(barrier, len(peers))


def push(src, dst, sems, at, px, pc, pz):
    return pltpu.make_async_remote_copy(
        src_ref=src,
        dst_ref=dst,
        send_sem=sems[0].at[at],
        recv_sem=sems[1].at[at],
        device_id={"ep": px * 2 + pc, "tp": pz},
        device_id_type=MESH,
    )


def gather_kernel(own_ref, out_ref, zs, zr, xs, xr, cs, cr):
    n_x, n_z, x, c, z = places()
    greet(n_x, n_z, x, c, z)
    z_sems, x_sems, c_sems = (zs, zr), (xs, xr), (cs, cr)
    sends = []

    def send(*what):
        copy = push(*what)
        copy.start()
        sends.append(copy)

    def place(d, k):
        return out_ref.at[(x - d + n_x) % n_x, c, (z - k + n_z) % n_z]

    def other(d, k):
        return out_ref.at[(x - d + n_x) % n_x, 1 - c, (z - k + n_z) % n_z]

    mine = out_ref.at[x, c, z]
    for k in range(1, n_z):
        send(own_ref, mine, z_sems, k - 1, x, c, (z + k) % n_z)
    for d in range(1, n_x):
        send(own_ref, mine, x_sems, (d - 1) * n_z, (x + d) % n_x, c, z)
    send(own_ref, mine, c_sems, 0, x, 1 - c, z)
    out_ref[x, c, z] = own_ref[...]
    for k in range(1, n_z):
        here = place(0, k)
        push(here, here, z_sems, k - 1, x, c, (z + k) % n_z).wait_recv()
        for d in range(1, n_x):
            send(here, here, x_sems, (d - 1) * n_z + k, (x + d) % n_x, c, z)
        send(here, here, c_sems, k, x, 1 - c, z)
    for k in range(n_z):
        for d in range(1, n_x):
            here = place(d, k)
            push(here, here, x_sems, (d - 1) * n_z + k, (x + d) % n_x, c, z).wait_recv()
            send(here, here, c_sems, d * n_z + k, x, 1 - c, z)
    for d in range(n_x):
        for k in range(n_z):
            there = other(d, k)
            push(there, there, c_sems, d * n_z + k, x, 1 - c, z).wait_recv()
    for copy in sends:
        copy.wait_send()


def gather(own):
    n_x, n_z = lax.axis_size("ep") // 2, lax.axis_size("tp")
    rows, width = own.shape
    sems = pltpu.SemaphoreType.DMA
    out = pl.pallas_call(
        gather_kernel,
        out_shape=jax.ShapeDtypeStruct((n_x, 2, n_z, rows, width), own.dtype),
        in_specs=[pl.BlockSpec(memory_space=pltpu.VMEM)],
        out_specs=pl.BlockSpec(memory_space=pltpu.VMEM),
        scratch_shapes=[sems((n_z,))] * 2 + [sems((n_x * n_z,))] * 4,
        compiler_params=pltpu.CompilerParams(
            collective_id=0, has_side_effects=True, vmem_limit_bytes=60 * 2**20
        ),
    )(own)
    return out.reshape(n_x * 2 * n_z * rows, width)


def scatter_kernel(part_ref, own_ref, out_ref, from_c, to_x, from_x, to_z, from_z, cs, cr, xs, xr, zs, zr):
    n_x, n_z, x, c, z = places()
    greet(n_x, n_z, x, c, z)
    c_sems, x_sems, z_sems = (cs, cr), (xs, xr), (zs, zr)
    sends = []

    def send(*what):
        copy = push(*what)
        copy.start()
        sends.append(copy)

    turns = list(range(1, n_z)) + [0]
    blocks = [(d, k) for d in list(range(1, n_x)) + [0] for k in turns]

    def pair_copy(d, k, side):
        src = part_ref.at[(x + d) % n_x, side, (z + k) % n_z]
        return src, from_c.at[d * n_z + k], c_sems, d * n_z + k, x, 1 - c, z

    for d, k in blocks:
        send(*pair_copy(d, k, 1 - c))

    def paired(d, k):
        push(*pair_copy(d, k, 1 - c)).wait_recv()
        near = part_ref[(x + d) % n_x, c, (z + k) % n_z].astype(jnp.float32)
        return near + from_c[d * n_z + k].astype(jnp.float32)

    for d in range(1, n_x):
        for k in turns:
            at = (d - 1) * n_z + k
            to_x[at] = paired(d, k).astype(to_x.dtype)
            send(to_x.at[at], from_x.at[at], x_sems, at, (x + d) % n_x, c, z)
    for k in turns:
        value = paired(0, k)
        for d in range(1, n_x):
            at = (d - 1) * n_z + k
            push(to_x.at[at], from_x.at[at], x_sems, at, (x + d) % n_x, c, z).wait_recv()
            value = value + from_x[at].astype(jnp.float32)
        if k:
            to_z[k - 1] = value.astype(to_z.dtype)
            send(to_z.at[k - 1], from_z.at[k - 1], z_sems, k - 1, x, c, (z + k) % n_z)
    for k in range(1, n_z):
        push(to_z.at[k - 1], from_z.at[k - 1], z_sems, k - 1, x, c, (z + k) % n_z).wait_recv()
        value = value + from_z[k - 1].astype(jnp.float32)
    out_ref[...] = (own_ref[...].astype(jnp.float32) + value).astype(out_ref.dtype)
    for copy in sends:
        copy.wait_send()


def scatter(part, own):
    n_x, n_z = lax.axis_size("ep") // 2, lax.axis_size("tp")
    rows, width = own.shape
    sems = pltpu.SemaphoreType.DMA
    held = [pltpu.VMEM((count, rows, width), part.dtype) for count in
            (n_x * n_z, (n_x - 1) * n_z, (n_x - 1) * n_z, n_z - 1, n_z - 1)]
    return pl.pallas_call(
        scatter_kernel,
        out_shape=jax.ShapeDtypeStruct(own.shape, own.dtype),
        in_specs=[pl.BlockSpec(memory_space=pltpu.VMEM)] * 2,
        out_specs=pl.BlockSpec(memory_space=pltpu.VMEM),
        scratch_shapes=held + [sems((n_x * n_z,))] * 4 + [sems((n_z,))] * 2,
        compiler_params=pltpu.CompilerParams(
            collective_id=1, has_side_effects=True, vmem_limit_bytes=60 * 2**20
        ),
    )(part.reshape(n_x, 2, n_z, rows, width), own)


def shards(hidden_states, norm_gain, expert_ids, gate_weights, capacity, expert_in, expert_out):
    token_count, width = hidden_states.shape
    expert_count = capacity.shape[0]
    local_count = expert_in.shape[0]
    values = hidden_states.astype(jnp.float32)
    inverse = lax.rsqrt(jnp.mean(values * values, axis=1, keepdims=True) + EPSILON)
    normed = (values * inverse * norm_gain).astype(jnp.bfloat16)
    lanes = jnp.arange(expert_count, dtype=jnp.int32)
    chosen = (expert_ids[:, :, None] == lanes).astype(jnp.float32)
    named = jnp.sum(chosen, axis=1)
    lower = jnp.tril(jnp.ones((token_count, token_count), jnp.float32), -1)
    before = jnp.dot(lower, named, precision=lax.Precision.HIGHEST)
    kept = before < capacity[None, :].astype(jnp.float32)
    gates = jnp.where(kept, jnp.sum(chosen * gate_weights[:, :, None], axis=1), 0.0)
    high = gates.astype(jnp.bfloat16)
    low = (gates - high.astype(jnp.float32)).astype(jnp.bfloat16)
    pad = jnp.zeros((token_count, 128 - 2 * expert_count), jnp.bfloat16)
    sent = jnp.concatenate([normed, high, low, pad], axis=1)
    gathered = gather(sent)
    high = gathered[:, width : width + expert_count].astype(jnp.float32)
    low = gathered[:, width + expert_count : width + 2 * expert_count].astype(jnp.float32)
    mine = lax.dynamic_slice_in_dim(high + low, lax.axis_index("ep") * local_count, local_count, 1)
    part = experts(gathered, width, mine.T, expert_in, expert_out)
    return scatter(part, hidden_states)


def solution(mesh):
    in_specs = (
        P(("groups", "ep", "tp"), None),
        P(),
        P(("groups", "ep", "tp"), None),
        P(("groups", "ep", "tp"), None),
        P(),
        P("ep", "tp", None, None),
        P("ep", "tp", None),
    )
    out_specs = P(("groups", "ep", "tp"), None)
    return jax.shard_map(shards, mesh=mesh, in_specs=in_specs, out_specs=out_specs, check_vma=False)
```
